512 devices in a mesh: blk: 512 (over x, y, z, core).
Axes of the slice: x: 4, y: 4, z: 16, core: 2. Of those that a mesh axis runs over, the one named last changes fastest.
Arguments:
- queries: bfloat16 [32768, 4096], P('blk'), may hold values from -200 to 200
- keys: bfloat16 [32768, 2048], P('blk'), may hold values from -8 to 8
- values: bfloat16 [32768, 2048], P('blk'), may hold values from -6 to 6
- doc_start: int32 [32768], P('blk'), may hold values from 0 to 32767, as said below
Outputs:
- attended: bfloat16 [32768, 4096], P('blk')
The draws below stay inside these ranges and needn't reach their ends.
Inputs may be any that keep to these rules, and one draw needn't show every extreme that they name: doc_start[i] is the first position of token i's document: nondecreasing, at most i, doc_start[doc_start[i]] = doc_start[i], and position 0 starts a document.
All inputs are finite; a program needn't handle non-finite values.
Results may differ from the reference program's by a relative error of at most 0.0034.
Values may be sent and summed in bfloat16 or wider, within the bound.
A program may use at most 64 MiB of HBM per device.

```python
import jax
import jax.numpy as jnp
from jax import lax

HEADS = 16
KV_HEADS = 8
HD = 256
TOK_DEV = 64
HOPS = 4
GROUP = 2
TOKENS = 32768


def drawn_pair(key):
    base = jax.random.fold_in(key, 11)
    key_q, key_k = jax.random.split(base, 2)
    key_vectors = jax.random.normal(key_k, (TOKENS, KV_HEADS * HD), jnp.float32)
    query_vectors = jax.random.normal(key_q, (TOKENS, HEADS * HD), jnp.float32)
    query_vectors = jnp.clip(query_vectors, -5.0, 5.0)
    key_vectors = jnp.clip(key_vectors, -5.0, 5.0)
    return (query_vectors, key_vectors)


def draw_queries(key, part):
    query_vectors, key_vectors = drawn_pair(key)
    return query_vectors.astype(jnp.bfloat16)


def draw_keys(key, part):
    query_vectors, key_vectors = drawn_pair(key)
    return key_vectors.astype(jnp.bfloat16)


def draw_doc_start(key, part):
    base = jax.random.fold_in(key, 23)
    key_kind, key_cut = jax.random.split(base)
    nblocks = TOKENS // TOK_DEV
    longer = jax.random.randint(key_kind, (nblocks,), 0, 2)
    period = jnp.where(longer == 1, 6 * TOK_DEV, 24).astype(jnp.int32)
    period = jnp.repeat(period, TOK_DEV)
    draws = jax.random.randint(key_cut, (TOKENS,), 0, 1 << 30)
    positions = jnp.arange(TOKENS, dtype=jnp.int32)
    boundary = (draws % period == 0) | (positions == 0)
    marks = jnp.where(boundary, positions, jnp.int32(0))
    return lax.cummax(marks, axis=0).astype(jnp.int32)


def block_scale(key, dims, cuts, low, top_value):
    level, own = 1.0, jax.random.fold_in(key, 6)
    for position, shards_of in cuts:
        heights = jnp.exp(jax.random.uniform(jax.random.fold_in(own, position), (shards_of,), jnp.float32, low / len(cuts), top_value / len(cuts)))
        level = level * jnp.repeat(heights, dims[position] // shards_of).reshape([-1 if axis == position else 1 for axis in range(len(dims))])
    return level


def bell_draw(own_key, extent, scale, reach, pieces=(), kind=jnp.bfloat16):
    drawn = jax.random.normal(own_key, extent, jnp.float32) * scale
    if len(pieces) > 0:
        drawn = block_scale(own_key, extent, pieces, -0.22, 0.18) * drawn
    return jnp.clip(drawn, min=-reach, max=reach).astype(kind)


def setup_inputs(seed: int = 0) -> dict:
    streams_of = jax.random.split(jax.random.key(seed), 5)
    return {
        "queries": draw_queries(jax.random.fold_in(streams_of[4], 71), 0),
        "keys": draw_keys(jax.random.fold_in(streams_of[4], 71), 0),
        "values": bell_draw(streams_of[2], (TOKENS, KV_HEADS * HD), 1.0, 6.0, ((0, 512),)),
        "doc_start": draw_doc_start(jax.random.fold_in(streams_of[4], 71), 0),
    }


def reference(queries, keys, values, doc_start):
    window = HOPS * TOK_DEV
    span = window + TOK_DEV
    key_pad = jnp.pad(keys, ((window, 0), (0, 0)))
    value_pad = jnp.pad(values, ((window, 0), (0, 0)))

    def one_block(index):
        start = (index * TOK_DEV).astype(jnp.int32)
        query_block = lax.dynamic_slice(queries, (start, jnp.int32(0)), (TOK_DEV, HEADS * HD))
        query_block = query_block.astype(jnp.float32).reshape(TOK_DEV, KV_HEADS, GROUP, HD)
        key_block = lax.dynamic_slice(key_pad, (start, jnp.int32(0)), (span, KV_HEADS * HD))
        key_block = key_block.astype(jnp.float32).reshape(span, KV_HEADS, HD)
        value_block = lax.dynamic_slice(value_pad, (start, jnp.int32(0)), (span, KV_HEADS * HD))
        value_block = value_block.astype(jnp.float32).reshape(span, KV_HEADS, HD)
        scores = jnp.einsum('qgrd,kgd->grqk', query_block, key_block) * 0.0625
        q_pos = start + jnp.arange(TOK_DEV, dtype=jnp.int32)
        k_pos = start - window + jnp.arange(span, dtype=jnp.int32)
        starts = lax.dynamic_slice(doc_start, (start,), (TOK_DEV,))
        allowed = (k_pos[None, :] <= q_pos[:, None]) & (q_pos[:, None] - k_pos[None, :] < window) & (k_pos[None, :] >= starts[:, None])
        scores = jnp.where(allowed, scores, jnp.float32(-1e30))
        top = jnp.max(scores, axis=-1, keepdims=True)
        expo = jnp.exp(scores - top)
        total = jnp.sum(expo, axis=-1)
        weights = lax.optimization_barrier(expo.astype(jnp.bfloat16)).astype(jnp.float32)
        mixed = jnp.einsum('grqk,kgd->qgrd', weights, value_block)
        mixed = mixed / jnp.transpose(total, (2, 0, 1))[..., None]
        return mixed.reshape(TOK_DEV, HEADS * HD).astype(jnp.bfloat16)

    blocks = lax.map(one_block, jnp.arange(TOKENS // TOK_DEV, dtype=jnp.int32))
    return blocks.reshape(TOKENS, HEADS * HD)
```

```python
import functools

import jax
import jax.numpy as jnp
from jax import lax
from jax.experimental import pallas as pl
from jax.experimental.pallas import tpu as pltpu
from jax.sharding import PartitionSpec as P

HD = 256
HOPS = 4
MESH = pl.DeviceIdType.MESH


def kernel(devices, rows, kv_heads, groups, q_hbm, k_hbm, v_hbm, starts_hbm, out_ref,
           q_ref, k_ref, v_ref, starts_ref, bias_ref, load_sem, own_send, near_recv, fwd_send, far_recv,
           a_send, a_recv, b_send, b_recv, misc_sem):
    me = lax.axis_index("blk")
    core = lax.rem(me, 2)
    ahead = lax.rem(me + 2, devices)
    behind = lax.rem(me + devices - 2, devices)
    partner = me + 1 - 2 * core
    span = (HOPS + 1) * rows

    barrier = pltpu.get_barrier_semaphore()
    for peer in (behind, partner):
        pl.semaphore_signal(barrier, inc=1, device_id=(peer,), device_id_type=MESH)

    pairs = ((k_hbm, k_ref), (v_hbm, v_ref))

    def columns(h):
        return pl.ds(pl.multiple_of(h * HD, HD), HD)

    def slot(index):
        return pl.ds(index * rows, rows)

    def load(h, t):
        source, target = pairs[t]
        return pltpu.make_async_copy(
            source.at[:, columns(h)], target.at[slot(HOPS), columns(h)], load_sem.at[2 * h + t])

    def remote(h, t, source_rows, target_rows, send, recv, device):
        ref = pairs[t][1]
        return pltpu.make_async_remote_copy(
            src_ref=ref.at[source_rows, columns(h)], dst_ref=ref.at[target_rows, columns(h)],
            send_sem=send.at[2 * h + t], recv_sem=recv.at[2 * h + t],
            device_id=(device,), device_id_type=MESH)

    def near(h, t):
        return remote(h, t, slot(4), slot(2), own_send, near_recv, ahead)

    def far(h, t):
        return remote(h, t, slot(2), slot(0), fwd_send, far_recv, ahead)

    def side_a(h, t):
        first = pl.multiple_of((4 - 2 * core) * rows, rows)
        return remote(h, t, pl.ds(first, rows), slot(3), a_send, a_recv, partner)

    def side_b(h, t):
        first = pl.multiple_of((2 - 2 * core) * rows, rows)
        return remote(h, t, pl.ds(first, rows), slot(1), b_send, b_recv, partner)

    starts_copy = pltpu.make_async_copy(starts_hbm, starts_ref, misc_sem.at[0])
    q_copy = pltpu.make_async_copy(q_hbm, q_ref, misc_sem.at[1])

    def start_load(h, carry):
        for t in range(2):
            load(h, t).start()
        return carry

    lax.fori_loop(0, kv_heads, start_load, 0)
    starts_copy.start()
    q_copy.start()
    pl.semaphore_wait(barrier, 2)

    def start_own(h, carry):
        for t in range(2):
            load(h, t).wait()
            near(h, t).start()

            @pl.when(core == 0)
            def _():
                side_a(h, t).start()
        return carry

    lax.fori_loop(0, kv_heads, start_own, 0)

    starts_copy.wait()
    row = lax.broadcasted_iota(jnp.int32, (rows, rows), 0)
    column = lax.broadcasted_iota(jnp.int32, (rows, rows), 1)
    spread = jnp.broadcast_to(starts_ref[...].astype(jnp.float32), (rows, rows))
    first = jnp.sum(jnp.where(row == column, spread, 0.0), axis=1, keepdims=True)
    start = me * rows
    q_pos = start + lax.broadcasted_iota(jnp.int32, (rows, span), 0)
    k_pos = start - HOPS * rows + lax.broadcasted_iota(jnp.int32, (rows, span), 1)
    allowed = (k_pos <= q_pos) & (q_pos - k_pos < HOPS * rows) & (k_pos.astype(jnp.float32) >= first)
    bias_ref[...] = jnp.where(allowed, 0.0, -1e30)
    q_copy.wait()

    def relay(h, carry):
        for t in range(2):
            near(h, t).wait_recv()
            far(h, t).start()

            @pl.when(core == 0)
            def _():
                side_b(h, t).start()

            @pl.when(core == 1)
            def _():
                side_a(h, t).start()
        return carry

    lax.fori_loop(0, kv_heads, relay, 0)

    def attend(h, carry):
        for t in range(2):
            far(h, t).wait_recv()

            @pl.when(core == 1)
            def _():
                side_b(h, t).start()
        for t in range(2):
            side_a(h, t).wait_recv()
            side_b(h, t).wait_recv()
        key = k_ref[:, columns(h)]
        value = v_ref[:, columns(h)]
        for g in range(groups):
            head = pl.ds(pl.multiple_of((h * groups + g) * HD, HD), HD)
            scores = lax.dot_general(
                q_ref[:, head], key, (((1,), (1,)), ((), ())), preferred_element_type=jnp.float32)
            scores = scores * 0.0625 + bias_ref[...]
            top = jnp.max(scores, axis=1, keepdims=True)
            expo = jnp.exp(scores - top)
            total = jnp.sum(expo, axis=1, keepdims=True)
            mixed = jnp.dot(expo.astype(jnp.bfloat16), value, preferred_element_type=jnp.float32)
            out_ref[:, head] = (mixed / total).astype(out_ref.dtype)
        return carry

    lax.fori_loop(0, kv_heads, attend, 0)

    def drain(h, carry):
        for t in range(2):
            near(h, t).wait_send()
            far(h, t).wait_send()
            side_a(h, t).wait_send()
            side_b(h, t).wait_send()
        return carry

    lax.fori_loop(0, kv_heads, drain, 0)


def per_device(devices, queries, keys, values, doc_start):
    rows = queries.shape[0]
    kv_heads = keys.shape[1] // HD
    groups = queries.shape[1] // keys.shape[1]
    span = (HOPS + 1) * rows
    copies = pltpu.SemaphoreType.DMA((2 * kv_heads,))
    return pl.pallas_call(
        functools.partial(kernel, devices, rows, kv_heads, groups),
        out_shape=jax.ShapeDtypeStruct(queries.shape, jnp.bfloat16),
        in_specs=[pl.BlockSpec(memory_space=pl.ANY)] * 4,
        out_specs=pl.BlockSpec(memory_space=pltpu.VMEM),
        scratch_shapes=[
            pltpu.VMEM(queries.shape, jnp.bfloat16),
            pltpu.VMEM((span, keys.shape[1]), jnp.bfloat16),
            pltpu.VMEM((span, keys.shape[1]), jnp.bfloat16),
            pltpu.VMEM((1, rows), jnp.int32),
            pltpu.VMEM((rows, span), jnp.float32),
            copies, copies, copies, copies, copies, copies, copies, copies, copies,
            pltpu.SemaphoreType.DMA((2,)),
        ],
        compiler_params=pltpu.CompilerParams(collective_id=0, has_side_effects=True),
    )(queries, keys, values, doc_start.reshape(1, rows))


def solution(mesh):
    return jax.shard_map(
        functools.partial(per_device, mesh.shape["blk"]),
        mesh=mesh,
        in_specs=(P("blk", None), P("blk", None), P("blk", None), P("blk")),
        out_specs=P("blk", None),
        check_vma=False,
    )
```

```python
import functools

import jax
import jax.numpy as jnp
from jax import lax
from jax.experimental import pallas as pl
from jax.experimental.pallas import tpu as pltpu
from jax.sharding import PartitionSpec as P

HD = 256
HOPS = 4
DEPTH = 16
MESH = pl.DeviceIdType.MESH


def kernel(devices, rows, kv_heads, groups, q_hbm, k_hbm, v_hbm, starts_hbm, out_ref,
           q_ref, k_ref, v_ref, k_pass, v_pass, starts_ref, bias_ref, load_sem, own_send, near_recv,
           fwd_send, far_recv, a_send, a_recv, b_send, b_recv, pass_send, pass_recv, misc_sem):
    me = lax.axis_index("blk")
    core = lax.rem(me, 2)
    chip = lax.div(me, 2)
    chips = devices // 2
    depth = lax.rem(chip, DEPTH)
    ahead = lax.rem(me + 2, devices)
    behind = lax.rem(me + devices - 2, devices)
    partner = me + 1 - 2 * core
    span = (HOPS + 1) * rows

    has_ahead = chip < chips - 1
    has_near = chip >= 1
    has_far = chip >= 2
    inner = chip < chips - DEPTH
    detour_first = inner & (depth == DEPTH - 2)
    detour_middle = inner & (depth == DEPTH // 2 - 1)
    detour_last = (depth == 0) & (chip > 0)
    short = inner & (depth == DEPTH - 1)
    to_middle = lax.rem(me + devices - DEPTH + 2, devices)
    to_last = lax.rem(me + DEPTH + 2, devices)

    @pl.when(chip < 2)
    def _():
        for ref in (k_ref, v_ref):
            ref[pl.ds(0, HOPS * rows), :] = jnp.zeros((HOPS * rows, ref.shape[1]), ref.dtype)

    barrier = pltpu.get_barrier_semaphore()

    def greet(peer):
        pl.semaphore_signal(barrier, inc=1, device_id=(peer,), device_id_type=MESH)

    greet(partner)

    @pl.when(has_near)
    def _():
        greet(behind)

    @pl.when(detour_middle)
    def _():
        greet(lax.rem(me + DEPTH - 2, devices))

    @pl.when(detour_last)
    def _():
        greet(lax.rem(me + devices - DEPTH - 2, devices))

    pairs = ((k_hbm, k_ref, k_pass), (v_hbm, v_ref, v_pass))

    def columns(h):
        return pl.ds(pl.multiple_of(h * HD, HD), HD)

    def slot(index):
        return pl.ds(index * rows, rows)

    def load(h, t):
        source, target, _ = pairs[t]
        return pltpu.make_async_copy(
            source.at[:, columns(h)], target.at[slot(HOPS), columns(h)], load_sem.at[2 * h + t])

    def remote(source, target, send, recv, device):
        return pltpu.make_async_remote_copy(
            src_ref=source, dst_ref=target, send_sem=send, recv_sem=recv,
            device_id=(device,), device_id_type=MESH)

    def between(h, t, source_rows, target_rows, send, recv, device):
        ref = pairs[t][1]
        return remote(ref.at[source_rows, columns(h)], ref.at[target_rows, columns(h)],
                      send.at[2 * h + t], recv.at[2 * h + t], device)

    def near(h, t):
        return between(h, t, slot(4), slot(2), own_send, near_recv, ahead)

    def far(h, t):
        return between(h, t, slot(2), slot(0), fwd_send, far_recv, ahead)

    def side_a(h, t):
        first = pl.multiple_of((4 - 2 * core) * rows, rows)
        return between(h, t, pl.ds(first, rows), slot(3), a_send, a_recv, partner)

    def side_b(h, t):
        first = pl.multiple_of((2 - 2 * core) * rows, rows)
        return between(h, t, pl.ds(first, rows), slot(1), b_send, b_recv, partner)

    def pass_in(j, t):
        _, ref, buffer = pairs[t]
        return remote(ref.at[slot(4), columns(2 * j + 1)], buffer.at[:, columns(j)],
                      pass_send.at[2 * j + t], pass_recv.at[2 * j + t], to_middle)

    def pass_out(j, t):
        _, ref, buffer = pairs[t]
        return remote(buffer.at[:, columns(j)], ref.at[slot(0), columns(2 * j + 1)],
                      pass_send.at[2 * j + t], far_recv.at[2 * (2 * j + 1) + t], to_last)

    starts_copy = pltpu.make_async_copy(starts_hbm, starts_ref, misc_sem.at[0])
    q_copy = pltpu.make_async_copy(q_hbm, q_ref, misc_sem.at[1])

    def start_load(h, carry):
        for t in range(2):
            load(h, t).start()
        return carry

    lax.fori_loop(0, kv_heads, start_load, 0)
    starts_copy.start()
    q_copy.start()

    awaited = 1 + has_ahead.astype(jnp.int32) + (detour_first | detour_middle).astype(jnp.int32)
    pl.semaphore_wait(barrier, awaited)

    def start_own(h, carry):
        for t in range(2):
            load(h, t).wait()

            @pl.when(has_ahead)
            def _():
                near(h, t).start()

            @pl.when(detour_first & (lax.rem(h, 2) == 1))
            def _():
                pass_in(lax.div(h, 2), t).start()

            @pl.when(core == 0)
            def _():
                side_a(h, t).start()
        return carry

    lax.fori_loop(0, kv_heads, start_own, 0)

    starts_copy.wait()
    row = lax.broadcasted_iota(jnp.int32, (rows, rows), 0)
    column = lax.broadcasted_iota(jnp.int32, (rows, rows), 1)
    spread = jnp.broadcast_to(starts_ref[...].astype(jnp.float32), (rows, rows))
    first = jnp.sum(jnp.where(row == column, spread, 0.0), axis=1, keepdims=True)
    start = me * rows
    q_pos = start + lax.broadcasted_iota(jnp.int32, (rows, span), 0)
    k_pos = start - HOPS * rows + lax.broadcasted_iota(jnp.int32, (rows, span), 1)
    allowed = (k_pos <= q_pos) & (q_pos - k_pos < HOPS * rows) & (k_pos.astype(jnp.float32) >= first)
    bias_ref[...] = jnp.where(allowed, 0.0, -1e30)
    q_copy.wait()

    def sends_far(h):
        return has_near & has_ahead & jnp.logical_not(short & (lax.rem(h, 2) == 1))

    def relay(h, carry):
        for t in range(2):
            @pl.when(has_near)
            def _():
                near(h, t).wait_recv()

            @pl.when(sends_far(h))
            def _():
                far(h, t).start()

            @pl.when(has_near & (core == 0))
            def _():
                side_b(h, t).start()

            @pl.when(has_near & (core == 1))
            def _():
                side_a(h, t).start()

        @pl.when(detour_middle & (h >= kv_heads - kv_heads // 2))
        def _():
            for t in range(2):
                pass_in(h - (kv_heads - kv_heads // 2), t).wait_recv()
                pass_out(h - (kv_heads - kv_heads // 2), t).start()
        return carry

    lax.fori_loop(0, kv_heads, relay, 0)

    def attend(h, carry):
        for t in range(2):
            @pl.when(has_far)
            def _():
                far(h, t).wait_recv()

            @pl.when(has_far & (core == 1))
            def _():
                side_b(h, t).start()
        for t in range(2):
            @pl.when(has_near | (core == 1))
            def _():
                side_a(h, t).wait_recv()

            @pl.when(has_far | (has_near & (core == 1)))
            def _():
                side_b(h, t).wait_recv()
        key = k_ref[:, columns(h)]
        value = v_ref[:, columns(h)]
        for g in range(groups):
            head = pl.ds(pl.multiple_of((h * groups + g) * HD, HD), HD)
            scores = lax.dot_general(
                q_ref[:, head], key, (((1,), (1,)), ((), ())), preferred_element_type=jnp.float32)
            scores = scores * 0.0625 + bias_ref[...]
            top = jnp.max(scores, axis=1, keepdims=True)
            expo = jnp.exp(scores - top)
            total = jnp.sum(expo, axis=1, keepdims=True)
            mixed = jnp.dot(expo.astype(jnp.bfloat16), value, preferred_element_type=jnp.float32)
            out_ref[:, head] = (mixed / total).astype(out_ref.dtype)
        return carry

    lax.fori_loop(0, kv_heads, attend, 0)

    def drain(h, carry):
        for t in range(2):
            @pl.when(has_ahead)
            def _():
                near(h, t).wait_send()

            @pl.when(sends_far(h))
            def _():
                far(h, t).wait_send()

            @pl.when(has_near | (core == 0))
            def _():
                side_a(h, t).wait_send()

            @pl.when(has_far | (has_near & (core == 0)))
            def _():
                side_b(h, t).wait_send()

            @pl.when((detour_first | detour_middle) & (lax.rem(h, 2) == 1))
            def _():
                pass_in(lax.div(h, 2), t).wait_send()
        return carry

    lax.fori_loop(0, kv_heads, drain, 0)


def per_device(devices, queries, keys, values, doc_start):
    rows = queries.shape[0]
    kv_heads = keys.shape[1] // HD
    groups = queries.shape[1] // keys.shape[1]
    span = (HOPS + 1) * rows
    copies = pltpu.SemaphoreType.DMA((2 * kv_heads,))
    half = pltpu.SemaphoreType.DMA((kv_heads,))
    return pl.pallas_call(
        functools.partial(kernel, devices, rows, kv_heads, groups),
        out_shape=jax.ShapeDtypeStruct(queries.shape, jnp.bfloat16),
        in_specs=[pl.BlockSpec(memory_space=pltpu.HBM)] * 4,
        out_specs=pl.BlockSpec(memory_space=pltpu.VMEM),
        scratch_shapes=[
            pltpu.VMEM(queries.shape, jnp.bfloat16),
            pltpu.VMEM((span, keys.shape[1]), jnp.bfloat16),
            pltpu.VMEM((span, keys.shape[1]), jnp.bfloat16),
            pltpu.VMEM((rows, keys.shape[1] // 2), jnp.bfloat16),
            pltpu.VMEM((rows, keys.shape[1] // 2), jnp.bfloat16),
            pltpu.VMEM((1, rows), jnp.int32),
            pltpu.VMEM((rows, span), jnp.float32),
            copies, copies, copies, copies, copies, copies, copies, copies, copies, half, half,
            pltpu.SemaphoreType.DMA((2,)),
        ],
        compiler_params=pltpu.CompilerParams(
            collective_id=0, has_side_effects=True, vmem_limit_bytes=8 * 1024 * 1024),
    )(*(pltpu.with_memory_space_constraint(x, pltpu.HBM) for x in (queries, keys, values, doc_start.reshape(1, rows))))


def solution(mesh):
    return jax.shard_map(
        functools.partial(per_device, mesh.shape["blk"]),
        mesh=mesh,
        in_specs=(P("blk", None), P("blk", None), P("blk", None), P("blk")),
        out_specs=P("blk", None),
        check_vma=False,
    )
```
